32 devices in a mesh: dp: 8 (over z, x), rep: 4 (over y, core).
Axes of the slice: x: 2, y: 2, z: 4, core: 2. Of those that a mesh axis runs over, the one named last changes fastest.
Arguments:
- tokens: bfloat16 [8192, 2048], P(('rep', 'dp')), parts along dimension 0, may hold values from -12 to 12
- router: bfloat16 [8192, 8], P('rep'), parts along dimension 0, may hold values from -12 to 12
- w_gate: bfloat16 [8, 2048, 768], P('dp'), may hold values from -0.125 to 0.125
- w_up: bfloat16 [8, 2048, 768], P('dp'), may hold values from -0.125 to 0.125
- w_down: bfloat16 [8, 768, 2048], P('dp'), may hold values from -0.21875 to 0.21875
- picks: int32 [32, 32], P(('rep', 'dp')), parts along dimension 0, may hold values from 0 to 2047, as said below
Outputs:
- combined: bfloat16 [8192, 2048], P(('rep', 'dp')), parts along dimension 0
The draws below stay inside these ranges and needn't reach their ends.
There are 4 independent parts, one for each index of `rep`. The reference program is written for one: setup_inputs(seed, part) draws one part's arguments, and reference() takes and returns one part's arrays. A program takes and returns all parts, laid end to end along the dimension named above; an argument that names none is the same for every part. Nothing has to cross between parts.
Inputs may be any that keep to these rules, and one draw needn't show every extreme that they name: `picks`: row e holds 32 different tokens taken by expert e, sorted by the device that holds them (256 tokens each, in order); at most 6 of them lie among one device's tokens, and in every row exactly 6 lie among some device's tokens.
All inputs are finite; a program needn't handle non-finite values.
Results may differ from the reference program's by a relative error of at most 0.0062.
Values may be sent and summed in bfloat16 or wider, within the bound.
A program may use at most 64 MiB of HBM per device.

```python
import math
import jax
import jax.numpy as jnp
from jax import lax

D = 2048
FF = 768
TOK_DEV = 256
BASE = 4
EXPERTS = 8
CAP = 32
TOKENS = 2048


def draw_router(key, part):
    base = jax.random.normal(jax.random.fold_in(key, 21), (D, EXPERTS), jnp.float32)
    matrix = base * (1.0 / math.sqrt(D))
    return jnp.clip(matrix, -12.0, 12.0).astype(jnp.bfloat16)


def draw_tokens(key, part):
    values = jax.random.normal(jax.random.fold_in(key, 31), (TOKENS, D), jnp.float32)
    return jnp.clip(values, -12.0, 12.0).astype(jnp.bfloat16)


def draw_picks(key, part):
    key_pair, key_shift, key_order = jax.random.split(key, 3)
    half_base = BASE // 2
    pairing = jax.vmap(lambda subkey: jax.random.permutation(subkey, EXPERTS))(jax.random.split(key_pair, EXPERTS))
    offsets = jax.random.randint(key_shift, (EXPERTS, EXPERTS // 2), -half_base, half_base + 1)
    offsets = offsets.at[:, 0].set(half_base)
    paired = (jnp.concatenate([offsets, -offsets], axis=1) + BASE).astype(jnp.int32)
    rows_at = jnp.arange(EXPERTS, dtype=jnp.int32)[:, None]
    counts = jnp.zeros((EXPERTS, EXPERTS), jnp.int32).at[rows_at, pairing].set(paired)
    block_end = jnp.cumsum(counts, axis=1)
    starts = block_end - counts
    slot_pos = jnp.arange(CAP, dtype=jnp.int32)
    source_of = jnp.sum((slot_pos[None, :, None] >= block_end[:, None, :]).astype(jnp.int32), axis=2)
    within = slot_pos[None, :] - jnp.take_along_axis(starts, source_of, axis=1)
    scores = jax.random.randint(key_order, (EXPERTS, EXPERTS, TOK_DEV), 0, 1 << 30)
    shuffled = jnp.argsort(scores, axis=2, stable=True).astype(jnp.int32)
    shuffled_rows = shuffled.reshape(EXPERTS * EXPERTS, TOK_DEV)
    row_index = rows_at * EXPERTS + source_of
    local_pick = shuffled_rows[row_index, within]
    return (source_of * TOK_DEV + local_pick).astype(jnp.int32)


def steps_of(key, dims, shards, smallest, largest):
    level = 1.0
    for dim, blocks in shards:
        steps = jax.random.uniform(jax.random.fold_in(jax.random.fold_in(key, 6), dim), (blocks,), jnp.float32, smallest / len(shards), largest / len(shards))
        level = level * jnp.repeat(jnp.exp(steps), dims[dim] // blocks).reshape((-1,) + (1,) * (len(dims) - 1 - dim))
    return level


def scatter_about(own_key, shape, deviation, reach, cuts=(), kind=jnp.bfloat16):
    array = jax.random.normal(own_key, shape, jnp.float32) * deviation
    if len(cuts) > 0:
        array = steps_of(own_key, shape, cuts, -0.22, 0.18) * array
    return jnp.clip(array, min=-reach, max=reach).astype(kind)


def setup_inputs(seed: int = 0, part: int = 0) -> dict:
    arg_keys = jax.random.split(jax.random.key(seed), 7)
    own_keys = jax.random.split(jax.random.fold_in(arg_keys[6], part), 7)
    return {
        "tokens": draw_tokens(jax.random.fold_in(jax.random.fold_in(arg_keys[6], part), 71), part),
        "router": draw_router(jax.random.fold_in(jax.random.fold_in(arg_keys[6], part), 71), part),
        "w_gate": scatter_about(arg_keys[2], (EXPERTS, D, FF), D ** -0.5, 0.125, ((0, 8),)),
        "w_up": scatter_about(arg_keys[3], (EXPERTS, D, FF), D ** -0.5, 0.125, ((0, 8),)),
        "w_down": scatter_about(arg_keys[4], (EXPERTS, FF, D), FF ** -0.5, 0.21875, ((0, 8),)),
        "picks": draw_picks(jax.random.fold_in(jax.random.fold_in(arg_keys[6], part), 71), part),
    }


def reference(tokens, router, w_gate, w_up, w_down, picks):
    logits = jnp.dot(tokens, router, preferred_element_type=jnp.float32)
    shares = jax.nn.softmax(logits, axis=1)
    gates = (EXPERTS * jnp.take_along_axis(shares.T, picks, axis=1)).astype(jnp.bfloat16)

    def one_expert(inputs):
        gate_w, up_w, down_w, chosen_index, gate_row = inputs
        chosen = tokens[chosen_index]
        gate_act = jnp.dot(chosen, gate_w, preferred_element_type=jnp.float32)
        up_act = jnp.dot(chosen, up_w, preferred_element_type=jnp.float32)
        hidden = (gate_row.astype(jnp.float32)[:, None] * jax.nn.silu(gate_act) * up_act).astype(jnp.bfloat16)
        return jnp.dot(hidden, down_w, preferred_element_type=jnp.float32).astype(jnp.bfloat16)

    results = lax.map(one_expert, (w_gate, w_up, w_down, picks, gates))
    width = tokens.shape[1]
    combined = jnp.zeros((tokens.shape[0], width), jnp.float32).at[picks.reshape(-1)].add(
        results.reshape(-1, width).astype(jnp.float32))
    return combined.astype(jnp.bfloat16)
```

```python
import functools

import jax
import jax.numpy as jnp
from jax import lax
from jax.experimental import pallas as pl
from jax.experimental.pallas import tpu as pltpu
from jax.sharding import PartitionSpec as P

MESH = pl.DeviceIdType.MESH
MOST = 6
SUB = 8
PARTS = 4
FOLD = 3
F32 = jnp.float32
BF16 = jnp.bfloat16


def mm(a, b):
    return jnp.dot(a, b, preferred_element_type=F32)


def mm_t(a, b):
    return lax.dot_general(a, b, (((0,), (0,)), ((), ())), preferred_element_type=F32)


def kernel(
    n, first_half, tokens, router, w_gate, w_up, w_down, picks, out,
    tok, rout, wg, wu, wd, pk_own, pk_out, pk_in, x_out, x_in, y_out, y_in,
    load_sem, wg_sem, wu_sem,
    pk_send, pk_recv, x_send, x_recv, y_send, y_recv,
):
    me = lax.axis_index("dp")
    tok_dev, width = tok.shape
    cols = width // PARTS
    piece = cols // (FOLD + 1)
    wide = FOLD * piece
    cap = picks.shape[1]
    lanes = pk_out.shape[1]
    rows = n * SUB
    experts = rout.shape[0]

    def span(k):
        return pl.ds(k * cols, cols)

    def front(k):
        return pl.ds(k * cols, wide)

    def back(k):
        return pl.ds(k * cols + wide, piece)

    def fold(matrices, x):
        return jnp.concatenate([mm(m, x) for m in matrices], axis=1)

    def unfold(dot, matrices, x):
        return sum(dot(m, x[:, j * piece : (j + 1) * piece]) for j, m in enumerate(matrices))

    load_tok = pltpu.make_async_copy(tokens, tok, load_sem.at[0])
    load_rout = pltpu.make_async_copy(router, rout, load_sem.at[1])
    load_pk = pltpu.make_async_copy(picks, pk_own, load_sem.at[3])
    load_wd = pltpu.make_async_copy(w_down.at[0], wd, load_sem.at[2])
    load_wg = [
        pltpu.make_async_copy(w_gate.at[0, span(k)], wg.at[span(k)], wg_sem.at[k])
        for k in range(PARTS)
    ]
    load_wu = [
        pltpu.make_async_copy(w_up.at[0, span(k)], wu.at[span(k)], wu_sem.at[k])
        for k in range(PARTS)
    ]

    barrier = pltpu.get_barrier_semaphore()
    peers = [n - 1 - j - (n - 1 - j <= me).astype(jnp.int32) for j in range(n - 1)]
    for peer in peers:
        pl.semaphore_signal(barrier, inc=1, device_id={"dp": peer}, device_id_type=MESH)
    load_pk.start()
    load_tok.start()
    load_rout.start()
    for k in range(PARTS):
        load_wg[k].start()
        load_wu[k].start()
    load_wd.start()

    pk_out[...] = jnp.full((SUB, lanes), 1 << 30, jnp.int32)
    load_pk.wait()
    pk_out[:, pl.ds(0, cap)] = jnp.broadcast_to(pk_own[...], (SUB, cap))
    pk_in[me] = pk_out[...]
    pl.semaphore_wait(barrier, n - 1)

    def send(src, dst, send_sem, recv_sem, peer):
        return pltpu.make_async_remote_copy(
            src_ref=src, dst_ref=dst, send_sem=send_sem, recv_sem=recv_sem,
            device_id={"dp": peer}, device_id_type=MESH,
        )

    pk_copies = [
        send(pk_out, pk_in.at[me], pk_send.at[peer], pk_recv.at[me], peer)
        for i, peer in enumerate(peers)
    ]
    for copy in pk_copies:
        copy.start()
    pk_waits = [
        send(pk_out, pk_in.at[peer], pk_send.at[peer], pk_recv.at[peer], peer)
        for i, peer in enumerate(peers)
    ]

    row_sub = lax.broadcasted_iota(jnp.int32, (rows, 1), 0) % SUB
    r_i = lax.broadcasted_iota(jnp.int32, (rows, rows), 0)
    q_i = lax.broadcasted_iota(jnp.int32, (rows, rows), 1)
    same = r_i // SUB == q_i // SUB
    spread = []
    gather = []
    for k in range(FOLD):
        a = (r_i % SUB == k) & (q_i % SUB == MOST)
        b = (r_i % SUB == FOLD + k) & (q_i % SUB == MOST + 1)
        spread.append(jnp.where(same & (a | b), 1.0, 0.0).astype(BF16))
        a = (q_i % SUB == k) & (r_i % SUB == MOST)
        b = (q_i % SUB == FOLD + k) & (r_i % SUB == MOST + 1)
        gather.append(jnp.where(same & (a | b), 1.0, 0.0).astype(BF16))
    load_tok.wait()

    low = me * tok_dev

    def choose(pk):
        count = pk.shape[0]
        mine = (pk >= low) & (pk < low + tok_dev)
        start = jnp.sum(jnp.where(pk < low, 1.0, 0.0), axis=1, keepdims=True).astype(jnp.int32)
        slot = lax.broadcasted_iota(jnp.int32, (count, lanes), 1) - start
        place = (pk - low + 1).astype(F32)
        token_at = lax.broadcasted_iota(jnp.int32, (count, tok_dev), 1).astype(F32) + 1.0
        sub = lax.broadcasted_iota(jnp.int32, (count, 1), 0) % SUB

        def onehot(slot_of_row):
            at = jnp.sum(jnp.where(mine & (slot == slot_of_row), place, 0.0), axis=1, keepdims=True)
            return jnp.where(token_at == at, 1.0, 0.0).astype(BF16)

        return [onehot(sub)] + [
            onehot(jnp.where(sub == MOST, k, jnp.where(sub == MOST + 1, FOLD + k, -1)))
            for k in range(FOLD)
        ]

    x_copies = [
        [
            send(x_out.at[k, peer], x_in.at[k, me], x_send.at[k, peer], x_recv.at[k, me], peer)
            for i, peer in enumerate(peers)
        ]
        for k in range(PARTS)
    ]
    x_waits = [
        [
            send(x_out.at[k, peer], x_in.at[k, peer], x_send.at[k, peer], x_recv.at[k, peer], peer)
            for i, peer in enumerate(peers)
        ]
        for k in range(PARTS)
    ]
    turn = n - first_half - 1
    chosen = []
    for lo, hi, js, cond in (
        (first_half, n, range(0, turn), me < first_half),
        (0, first_half, range(turn + 1, n - 1), me >= first_half),
    ):
        for j in js:
            pk_waits[j].wait_recv()

        @pl.when(cond)
        def _():
            pk_waits[turn].wait_recv()

        hots = choose(pk_in[lo:hi].reshape((hi - lo) * SUB, lanes))
        chosen.append(hots)
        for k in range(PARTS):
            block = mm(hots[0], tok[:, front(k)]) + fold(hots[1:], tok[:, back(k)])
            x_out[k, lo:hi] = block.astype(BF16).reshape(hi - lo, SUB, wide)
            for j in js:
                x_copies[k][j].start()

            @pl.when(cond)
            def _(k=k):
                x_copies[k][turn].start()

    for k in range(PARTS):
        x_in[k, me] = x_out[k, me]
    main, *tails = [jnp.concatenate(hots, axis=0) for hots in zip(*chosen[::-1])]

    gate_act = up_act = logits = None

    def total(a, b):
        return b if a is None else a + b

    def step(x, k):
        dims = (((1,), (1,)), ((), ()))
        return (
            total(gate_act, mm(x, wg[span(k)])),
            total(up_act, mm(x, wu[span(k)])),
            total(logits, lax.dot_general(x, rout[:, span(k)], dims, preferred_element_type=F32)),
        )

    load_rout.wait()
    for k in range(PARTS):
        load_wg[k].wait()
        load_wu[k].wait()
        for copy in x_waits[k]:
            copy.wait_recv()
        x = x_in[k].reshape(rows, wide)
        x = jnp.concatenate([x, unfold(mm, spread, x).astype(BF16)], axis=1)
        gate_act, up_act, logits = step(x, k)

    e = jnp.exp(logits - jnp.max(logits, axis=1, keepdims=True))
    own = lax.broadcasted_iota(jnp.int32, (rows, experts), 1) == me
    share = jnp.sum(jnp.where(own, e, 0.0), axis=1, keepdims=True) / jnp.sum(e, axis=1, keepdims=True)
    gates = (experts * share).astype(BF16).astype(F32)
    silu = gate_act / (1.0 + jnp.exp(-gate_act))
    hidden = (gates * silu * up_act).astype(BF16)

    load_wd.wait()
    y_copies = [
        [
            send(y_out.at[k, peer], y_in.at[k, me], y_send.at[k, peer], y_recv.at[k, me], peer)
            for i, peer in enumerate(peers)
        ]
        for k in range(PARTS)
    ]
    for k in range(PARTS):
        block = mm(hidden, wd[:, span(k)])
        block = jnp.where(row_sub < MOST, block[:, :wide], fold(gather, block[:, wide:].astype(BF16)))
        y_out[k] = block.astype(BF16).reshape(n, SUB, wide)
        y_in[k, me] = y_out[k, me]
        for copy in y_copies[k][::-1]:
            copy.start()

    y_waits = [
        [
            send(y_out.at[k, peer], y_in.at[k, peer], y_send.at[k, peer], y_recv.at[k, peer], peer)
            for i, peer in enumerate(peers)
        ]
        for k in range(PARTS)
    ]
    for k in range(PARTS):
        for copy in y_waits[k]:
            copy.wait_recv()
        y = y_in[k].reshape(rows, wide)
        out[:, front(k)] = mm_t(main, y).astype(BF16)
        out[:, back(k)] = unfold(mm_t, tails, y).astype(BF16)
    for copies in [pk_copies] + x_copies + y_copies:
        for copy in copies:
            copy.wait_send()


def body(tokens, router, w_gate, w_up, w_down, picks):
    n = lax.axis_size("dp")
    tok_dev, width = tokens.shape
    hidden = w_gate.shape[2]
    wide = width // PARTS * FOLD // (FOLD + 1)
    cap = picks.shape[1]
    lanes = -(-cap // 128) * 128
    experts = router.shape[1]
    dma = pltpu.SemaphoreType.DMA
    block = pltpu.VMEM((PARTS, n, SUB, wide), BF16)
    return pl.pallas_call(
        functools.partial(kernel, n, n // 2),
        out_shape=pltpu.VMEM((tok_dev, width), BF16),
        in_specs=[pl.BlockSpec(memory_space=pl.ANY)] * 6,
        out_specs=pl.BlockSpec(memory_space=pltpu.VMEM),
        scratch_shapes=[
            pltpu.VMEM((tok_dev, width), BF16),
            pltpu.VMEM((experts, width), BF16),
            pltpu.VMEM((width, hidden), BF16),
            pltpu.VMEM((width, hidden), BF16),
            pltpu.VMEM((hidden, width), BF16),
            pltpu.VMEM((1, cap), jnp.int32),
            pltpu.VMEM((SUB, lanes), jnp.int32),
            pltpu.VMEM((n, SUB, lanes), jnp.int32),
            block, block, block, block,
            dma((4,)), dma((PARTS,)), dma((PARTS,)),
            dma((n,)), dma((n,)),
            dma((PARTS, n)), dma((PARTS, n)),
            dma((PARTS, n)), dma((PARTS, n)),
        ],
        compiler_params=pltpu.CompilerParams(collective_id=0, has_side_effects=True),
    )(tokens, router.T, w_gate, w_up, w_down, picks)


def solution(mesh):
    return jax.shard_map(
        body,
        mesh=mesh,
        in_specs=(
            P(("rep", "dp"), None),
            P("rep", None),
            P("dp", None, None),
            P("dp", None, None),
            P("dp", None, None),
            P(("rep", "dp"), None),
        ),
        out_specs=P(("rep", "dp"), None),
        check_vma=False,
    )
```

```python
import functools

import jax
import jax.numpy as jnp
from jax import lax
from jax.experimental import pallas as pl
from jax.experimental.pallas import tpu as pltpu
from jax.sharding import PartitionSpec as P

MESH = pl.DeviceIdType.MESH
PAIRS = 3
LOADS = 4
X_PARTS = 2
Y_PARTS = 2
F32 = jnp.float32
BF16 = jnp.bfloat16


def mm(a, b):
    return jnp.dot(a, b, preferred_element_type=F32)


def mm_t(a, b):
    return lax.dot_general(a, b, (((0,), (0,)), ((), ())), preferred_element_type=F32)


def kernel(
    n, tokens, router, w_gate, w_up, w_down, picks, out,
    tok, rout, wg, wu, wd, pk_own, pk_out, pk_in, x_out, x_in, y_out, y_in,
    load_sem, wg_sem, wu_sem,
    pk_send, pk_recv, x_send, x_recv, y_send, y_recv,
):
    me = lax.axis_index("dp")
    tok_dev, width = tok.shape
    cap = picks.shape[1]
    lanes = pk_out.shape[1]
    experts = rout.shape[0]
    half = n // 2

    def span(k, parts):
        return pl.ds(k * (width // parts), width // parts)

    def rows_of(ref):
        groups = [ref[:, i].reshape(2 * n, ref.shape[-1]) for i in range(PAIRS)]
        return jnp.concatenate(groups, axis=0)

    load_tok = pltpu.make_async_copy(tokens, tok, load_sem.at[0])
    load_rout = pltpu.make_async_copy(router, rout, load_sem.at[1])
    load_pk = pltpu.make_async_copy(picks, pk_own, load_sem.at[3])
    load_wd = pltpu.make_async_copy(w_down.at[0], wd, load_sem.at[2])
    load_wg = [
        pltpu.make_async_copy(w_gate.at[0, span(k, LOADS)], wg.at[span(k, LOADS)], wg_sem.at[k])
        for k in range(LOADS)
    ]
    load_wu = [
        pltpu.make_async_copy(w_up.at[0, span(k, LOADS)], wu.at[span(k, LOADS)], wu_sem.at[k])
        for k in range(LOADS)
    ]

    barrier = pltpu.get_barrier_semaphore()
    peers = [n - 1 - j - (n - 1 - j <= me).astype(jnp.int32) for j in range(n - 1)]
    for peer in peers:
        pl.semaphore_signal(barrier, inc=1, device_id={"dp": peer}, device_id_type=MESH)
    load_pk.start()
    load_tok.start()
    load_rout.start()
    for k in range(LOADS):
        load_wg[k].start()
        load_wu[k].start()
    load_wd.start()

    pk_out[...] = jnp.full((2, lanes), 1 << 30, jnp.int32)
    load_pk.wait()
    pk_out[:, pl.ds(0, cap)] = jnp.broadcast_to(pk_own[...], (2, cap))
    pk_in[me] = pk_out[...]
    pl.semaphore_wait(barrier, n - 1)

    def copy_of(src, dst, send_sem, recv_sem, peer):
        return pltpu.make_async_remote_copy(
            src_ref=src, dst_ref=dst, send_sem=send_sem, recv_sem=recv_sem,
            device_id={"dp": peer}, device_id_type=MESH,
        )

    def exchange(src, dst, send_sem, recv_sem):
        puts = [copy_of(src.at[p], dst.at[me], send_sem.at[p], recv_sem.at[me], p) for p in peers]
        gets = [copy_of(src.at[p], dst.at[p], send_sem.at[p], recv_sem.at[p], p) for p in peers]
        return puts, gets

    pk_puts = [copy_of(pk_out, pk_in.at[me], pk_send.at[p], pk_recv.at[me], p) for p in peers]
    pk_gets = [copy_of(pk_out, pk_in.at[p], pk_send.at[p], pk_recv.at[p], p) for p in peers]
    for put in pk_puts:
        put.start()

    load_tok.wait()
    load_rout.wait()
    logits = lax.dot_general(
        rout[...], tok[...], (((1,), (1,)), ((), ())), preferred_element_type=F32
    )
    e = jnp.exp(logits - jnp.max(logits, axis=0, keepdims=True))
    gates = (experts * (e / jnp.sum(e, axis=0, keepdims=True))).astype(BF16).astype(F32)

    low = me * tok_dev

    def choose(first, last):
        pk = pk_in[first:last].reshape(2 * (last - first), lanes)
        pk = jnp.concatenate([pk] * PAIRS, axis=0)
        count = pk.shape[0]
        mine = (pk >= low) & (pk < low + tok_dev)
        start = jnp.sum(jnp.where(pk < low, 1.0, 0.0), axis=1, keepdims=True).astype(jnp.int32)
        slot = lax.broadcasted_iota(jnp.int32, (count, lanes), 1) - start
        place = (pk - low + 1).astype(F32)
        row = lax.broadcasted_iota(jnp.int32, (count, 1), 0)
        want = 2 * (row // (count // PAIRS)) + row % 2
        at = jnp.sum(jnp.where(mine & (slot == want), place, 0.0), axis=1, keepdims=True)
        token_at = lax.broadcasted_iota(jnp.int32, (count, tok_dev), 1).astype(F32) + 1.0
        return jnp.where(token_at == at, 1.0, 0.0)

    x_puts, x_gets = zip(*[
        exchange(x_out.at[k], x_in.at[k], x_send.at[k], x_recv.at[k]) for k in range(X_PARTS)
    ])
    y_puts, y_gets = zip(*[
        exchange(y_out.at[k], y_in.at[k], y_send.at[k], y_recv.at[k]) for k in range(Y_PARTS)
    ])
    turn = half - 1
    for first, last, js, also in (
        (n - half, n, range(turn), me < n - half),
        (0, n - half, range(turn + 1, n - 1), me >= n - half),
    ):
        for j in js:
            pk_gets[j].wait_recv()

        @pl.when(also)
        def _():
            pk_gets[turn].wait_recv()

        size = 2 * (last - first)
        hot = choose(first, last).astype(BF16)
        for k in range(X_PARTS):
            block = mm(hot, tok[:, span(k, X_PARTS)])
            for i in range(PAIRS):
                rows = block[i * size : (i + 1) * size].astype(BF16)
                x_out[k, first:last, i] = rows.reshape(last - first, 2, rows.shape[1])
            for j in js:
                x_puts[k][j].start()

            @pl.when(also)
            def _(k=k):
                x_puts[k][turn].start()

    for k in range(X_PARTS):
        x_in[k, me] = x_out[k, me]
    gate_of = jnp.broadcast_to(gates[:, None, :], (n, 2, tok_dev)).reshape(2 * n, tok_dev)
    spread = (choose(0, n) * jnp.concatenate([gate_of] * PAIRS, axis=0)).T.astype(BF16)

    for copy in load_wg + load_wu:
        copy.wait()
    gate_act = up_act = None
    for k in range(X_PARTS):
        for get in x_gets[k]:
            get.wait_recv()
        x = rows_of(x_in.at[k])
        gate_part = mm(x, wg[span(k, X_PARTS)])
        up_part = mm(x, wu[span(k, X_PARTS)])
        gate_act = gate_part if k == 0 else gate_act + gate_part
        up_act = up_part if k == 0 else up_act + up_part
    hidden = (gate_act / (1.0 + jnp.exp(-gate_act)) * up_act).astype(BF16)

    load_wd.wait()
    for k in range(Y_PARTS):
        block = mm(hidden, wd[:, span(k, Y_PARTS)]).astype(BF16)
        for i in range(PAIRS):
            rows = block[i * 2 * n : (i + 1) * 2 * n]
            y_out[k, :, i] = rows.reshape(n, 2, rows.shape[1])
        for put in y_puts[k][::-1][:1]:
            put.start()
        y_in[k, me] = y_out[k, me]
    for k in range(Y_PARTS):
        for put in y_puts[k][::-1][1:]:
            put.start()

    for puts in [pk_puts, *x_puts]:
        for put in puts:
            put.wait_send()
    for k in range(Y_PARTS):
        for get in y_gets[k]:
            get.wait_recv()
        out[:, span(k, Y_PARTS)] = mm(spread, rows_of(y_in.at[k])).astype(BF16)
    for puts in y_puts:
        for put in puts:
            put.wait_send()


def body(tokens, router, w_gate, w_up, w_down, picks):
    n = lax.axis_size("dp")
    tok_dev, width = tokens.shape
    hidden = w_gate.shape[2]
    cap = picks.shape[1]
    lanes = -(-cap // 128) * 128
    experts = router.shape[1]
    dma = pltpu.SemaphoreType.DMA
    x_block = pltpu.VMEM((X_PARTS, n, PAIRS, 2, width // X_PARTS), BF16)
    y_block = pltpu.VMEM((Y_PARTS, n, PAIRS, 2, width // Y_PARTS), BF16)
    return pl.pallas_call(
        functools.partial(kernel, n),
        out_shape=pltpu.VMEM((tok_dev, width), BF16),
        in_specs=[pl.BlockSpec(memory_space=pl.ANY)] * 6,
        out_specs=pl.BlockSpec(memory_space=pltpu.VMEM),
        scratch_shapes=[
            pltpu.VMEM((tok_dev, width), BF16),
            pltpu.VMEM((experts, width), BF16),
            pltpu.VMEM((width, hidden), BF16),
            pltpu.VMEM((width, hidden), BF16),
            pltpu.VMEM((hidden, width), BF16),
            pltpu.VMEM((1, cap), jnp.int32),
            pltpu.VMEM((2, lanes), jnp.int32),
            pltpu.VMEM((n, 2, lanes), jnp.int32),
            x_block, x_block, y_block, y_block,
            dma((4,)), dma((LOADS,)), dma((LOADS,)),
            dma((n,)), dma((n,)),
            dma((X_PARTS, n)), dma((X_PARTS, n)),
            dma((Y_PARTS, n)), dma((Y_PARTS, n)),
        ],
        compiler_params=pltpu.CompilerParams(collective_id=0, has_side_effects=True),
    )(tokens, router.T, w_gate, w_up, w_down, picks)


def solution(mesh):
    return jax.shard_map(
        body,
        mesh=mesh,
        in_specs=(
            P(("rep", "dp"), None),
            P("rep", None),
            P("dp", None, None),
            P("dp", None, None),
            P("dp", None, None),
            P(("rep", "dp"), None),
        ),
        out_specs=P(("rep", "dp"), None),
        check_vma=False,
    )
```

```python
import functools

import jax
import jax.numpy as jnp
from jax import lax
from jax.experimental import pallas as pl
from jax.experimental.pallas import tpu as pltpu
from jax.sharding import PartitionSpec as P

MESH = pl.DeviceIdType.MESH
PAIRS = 3
LOADS = 4
X_PARTS = 2
Y_PARTS = 2
F32 = jnp.float32
BF16 = jnp.bfloat16


def mm(a, b):
    return jnp.dot(a, b, preferred_element_type=F32)


def mm_t(a, b):
    return lax.dot_general(a, b, (((0,), (0,)), ((), ())), preferred_element_type=F32)


def kernel(
    n, tokens, router, w_gate, w_up, w_down, picks, out,
    tok, rout, wg, wu, wd, pk_own, pk_out, pk_in, x_out, x_in, y_out, y_in,
    load_sem, wg_sem, wu_sem,
    pk_send, pk_recv, x_send, x_recv, y_send, y_recv,
):
    me = lax.axis_index("dp")
    tok_dev, width = tok.shape
    cap = picks.shape[1]
    lanes = pk_out.shape[1]
    experts = rout.shape[0]
    half = n // 2

    def span(k, parts):
        return pl.ds(k * (width // parts), width // parts)

    def rows_of(ref):
        groups = [ref[:, i].reshape(2 * ref.shape[0], ref.shape[-1]) for i in range(PAIRS)]
        return jnp.concatenate(groups, axis=0)

    load_tok = pltpu.make_async_copy(tokens, tok, load_sem.at[0])
    load_rout = pltpu.make_async_copy(router, rout, load_sem.at[1])
    load_pk = pltpu.make_async_copy(picks, pk_own, load_sem.at[3])
    load_wd = pltpu.make_async_copy(w_down.at[0], wd, load_sem.at[2])
    load_wg = [
        pltpu.make_async_copy(w_gate.at[0, span(k, LOADS)], wg.at[span(k, LOADS)], wg_sem.at[k])
        for k in range(LOADS)
    ]
    load_wu = [
        pltpu.make_async_copy(w_up.at[0, span(k, LOADS)], wu.at[span(k, LOADS)], wu_sem.at[k])
        for k in range(LOADS)
    ]

    barrier = pltpu.get_barrier_semaphore()
    peers = [n - 1 - j - (n - 1 - j <= me).astype(jnp.int32) for j in range(n - 1)]
    for peer in peers:
        pl.semaphore_signal(barrier, inc=1, device_id={"dp": peer}, device_id_type=MESH)
    load_pk.start()
    load_tok.start()
    load_rout.start()
    for k in range(LOADS):
        load_wg[k].start()
        load_wu[k].start()
    load_wd.start()

    pk_out[...] = jnp.full((2, lanes), 1 << 30, jnp.int32)
    load_pk.wait()
    pk_out[:, pl.ds(0, cap)] = jnp.broadcast_to(pk_own[...], (2, cap))
    pk_in[me] = pk_out[...]
    pl.semaphore_wait(barrier, n - 1)

    def copy_of(src, dst, send_sem, recv_sem, peer):
        return pltpu.make_async_remote_copy(
            src_ref=src, dst_ref=dst, send_sem=send_sem, recv_sem=recv_sem,
            device_id={"dp": peer}, device_id_type=MESH,
        )

    def exchange(src, dst, send_sem, recv_sem):
        puts = [copy_of(src.at[p], dst.at[me], send_sem.at[p], recv_sem.at[me], p) for p in peers]
        gets = [copy_of(src.at[p], dst.at[p], send_sem.at[p], recv_sem.at[p], p) for p in peers]
        return puts, gets

    pk_puts = [copy_of(pk_out, pk_in.at[me], pk_send.at[p], pk_recv.at[me], p) for p in peers]
    pk_gets = [copy_of(pk_out, pk_in.at[p], pk_send.at[p], pk_recv.at[p], p) for p in peers]
    for put in pk_puts:
        put.start()

    load_tok.wait()
    load_rout.wait()
    logits = lax.dot_general(
        rout[...], tok[...], (((1,), (1,)), ((), ())), preferred_element_type=F32
    )
    e = jnp.exp(logits - jnp.max(logits, axis=0, keepdims=True))
    gates = (experts * (e / jnp.sum(e, axis=0, keepdims=True))).astype(BF16).astype(F32)

    low = me * tok_dev

    def choose(first, last):
        pk = pk_in[first:last].reshape(2 * (last - first), lanes)
        pk = jnp.concatenate([pk] * PAIRS, axis=0)
        count = pk.shape[0]
        mine = (pk >= low) & (pk < low + tok_dev)
        start = jnp.sum(jnp.where(pk < low, 1.0, 0.0), axis=1, keepdims=True).astype(jnp.int32)
        slot = lax.broadcasted_iota(jnp.int32, (count, lanes), 1) - start
        place = (pk - low + 1).astype(F32)
        row = lax.broadcasted_iota(jnp.int32, (count, 1), 0)
        want = 2 * (row // (count // PAIRS)) + row % 2
        at = jnp.sum(jnp.where(mine & (slot == want), place, 0.0), axis=1, keepdims=True)
        token_at = lax.broadcasted_iota(jnp.int32, (count, tok_dev), 1).astype(F32) + 1.0
        return jnp.where(token_at == at, 1.0, 0.0)

    x_puts, x_gets = zip(*[
        exchange(x_out.at[k], x_in.at[k], x_send.at[k], x_recv.at[k]) for k in range(X_PARTS)
    ])
    y_puts, y_gets = zip(*[
        exchange(y_out.at[k], y_in.at[k], y_send.at[k], y_recv.at[k]) for k in range(Y_PARTS)
    ])
    turn = half - 1
    sides = (
        (n - half, n, range(turn), me < n - half),
        (0, n - half, range(turn + 1, n - 1), me >= n - half),
    )
    for first, last, js, also in sides:
        for j in js:
            pk_gets[j].wait_recv()

        @pl.when(also)
        def _():
            pk_gets[turn].wait_recv()

        size = 2 * (last - first)
        hot = choose(first, last).astype(BF16)
        for k in range(X_PARTS):
            block = mm(hot, tok[:, span(k, X_PARTS)])
            for i in range(PAIRS):
                rows = block[i * size : (i + 1) * size].astype(BF16)
                x_out[k, first:last, i] = rows.reshape(last - first, 2, rows.shape[1])
            for j in js:
                x_puts[k][j].start()

            @pl.when(also)
            def _(k=k):
                x_puts[k][turn].start()

    for k in range(X_PARTS):
        x_in[k, me] = x_out[k, me]
    gate_of = jnp.broadcast_to(gates[:, None, :], (n, 2, tok_dev)).reshape(2 * n, tok_dev)
    spread = (choose(0, n) * jnp.concatenate([gate_of] * PAIRS, axis=0)).T.astype(BF16)

    for copy in load_wg + load_wu:
        copy.wait()
    load_wd.wait()
    for first, last, js, also in sides[::-1]:
        size = 2 * (last - first)
        gate_act = up_act = None
        for k in range(X_PARTS):
            for j in js:
                x_gets[k][j].wait_recv()

            @pl.when(also)
            def _(k=k):
                x_gets[k][turn].wait_recv()

            x = rows_of(x_in.at[k, first:last])
            gate_part = mm(x, wg[span(k, X_PARTS)])
            up_part = mm(x, wu[span(k, X_PARTS)])
            gate_act = gate_part if k == 0 else gate_act + gate_part
            up_act = up_part if k == 0 else up_act + up_part
        hidden = (gate_act / (1.0 + jnp.exp(-gate_act)) * up_act).astype(BF16)
        for k in range(Y_PARTS):
            block = mm(hidden, wd[:, span(k, Y_PARTS)])
            for i in range(PAIRS):
                rows = block[i * size : (i + 1) * size].astype(BF16)
                y_out[k, first:last, i] = rows.reshape(last - first, 2, rows.shape[1])
            for j in reversed(js):
                y_puts[k][j].start()

            @pl.when(also)
            def _(k=k):
                y_puts[k][turn].start()

    for k in range(Y_PARTS):
        y_in[k, me] = y_out[k, me]

    for puts in [pk_puts, *x_puts]:
        for put in puts:
            put.wait_send()
    for k in range(Y_PARTS):
        for get in y_gets[k]:
            get.wait_recv()
        out[:, span(k, Y_PARTS)] = mm(spread, rows_of(y_in.at[k])).astype(BF16)
    for puts in y_puts:
        for put in puts:
            put.wait_send()


def body(tokens, router, w_gate, w_up, w_down, picks):
    n = lax.axis_size("dp")
    tok_dev, width = tokens.shape
    hidden = w_gate.shape[2]
    cap = picks.shape[1]
    lanes = -(-cap // 128) * 128
    experts = router.shape[1]
    dma = pltpu.SemaphoreType.DMA
    x_block = pltpu.VMEM((X_PARTS, n, PAIRS, 2, width // X_PARTS), BF16)
    y_block = pltpu.VMEM((Y_PARTS, n, PAIRS, 2, width // Y_PARTS), BF16)
    return pl.pallas_call(
        functools.partial(kernel, n),
        out_shape=pltpu.VMEM((tok_dev, width), BF16),
        in_specs=[pl.BlockSpec(memory_space=pl.ANY)] * 6,
        out_specs=pl.BlockSpec(memory_space=pltpu.VMEM),
        scratch_shapes=[
            pltpu.VMEM((tok_dev, width), BF16),
            pltpu.VMEM((experts, width), BF16),
            pltpu.VMEM((width, hidden), BF16),
            pltpu.VMEM((width, hidden), BF16),
            pltpu.VMEM((hidden, width), BF16),
            pltpu.VMEM((1, cap), jnp.int32),
            pltpu.VMEM((2, lanes), jnp.int32),
            pltpu.VMEM((n, 2, lanes), jnp.int32),
            x_block, x_block, y_block, y_block,
            dma((4,)), dma((LOADS,)), dma((LOADS,)),
            dma((n,)), dma((n,)),
            dma((X_PARTS, n)), dma((X_PARTS, n)),
            dma((Y_PARTS, n)), dma((Y_PARTS, n)),
        ],
        compiler_params=pltpu.CompilerParams(collective_id=0, has_side_effects=True),
    )(tokens, router.T, w_gate, w_up, w_down, picks)


def solution(mesh):
    return jax.shard_map(
        body,
        mesh=mesh,
        in_specs=(
            P(("rep", "dp"), None),
            P("rep", None),
            P("dp", None, None),
            P("dp", None, None),
            P("dp", None, None),
            P(("rep", "dp"), None),
        ),
        out_specs=P(("rep", "dp"), None),
        check_vma=False,
    )
```

```python
import functools

import jax
import jax.numpy as jnp
from jax import lax
from jax.experimental import pallas as pl
from jax.experimental.pallas import tpu as pltpu
from jax.sharding import PartitionSpec as P

MESH = pl.DeviceIdType.MESH
PAIRS = 3
LOADS = 4
X_CUTS = (0, 4, 8)
Y_CUTS = (0, 4, 8)
X_PARTS = len(X_CUTS) - 1
Y_PARTS = len(Y_CUTS) - 1
F32 = jnp.float32
BF16 = jnp.bfloat16


def mm(a, b):
    return jnp.dot(a, b, preferred_element_type=F32)


def mm_t(a, b):
    return lax.dot_general(a, b, (((0,), (0,)), ((), ())), preferred_element_type=F32)


def kernel(
    n, tokens, router, w_gate, w_up, w_down, picks, out,
    tok, rout, wg, wu, wd, pk_own, pk_out, pk_in, x_out, x_in, y_out, y_in,
    load_sem, wg_sem, wu_sem,
    pk_send, pk_recv, x_send, x_recv, y_send, y_recv,
):
    me = lax.axis_index("dp")
    tok_dev, width = tok.shape
    cap = picks.shape[1]
    lanes = pk_out.shape[1]
    experts = rout.shape[0]
    half = n // 2

    def span(k, parts):
        return pl.ds(k * (width // parts), width // parts)

    def cut(k, cuts):
        unit = width // cuts[-1]
        return pl.ds(cuts[k] * unit, (cuts[k + 1] - cuts[k]) * unit)

    def rows_of(ref, cols):
        groups = [ref[:, i, :, cols].reshape(2 * ref.shape[0], cols.size) for i in range(PAIRS)]
        return jnp.concatenate(groups, axis=0)

    load_tok = pltpu.make_async_copy(tokens, tok, load_sem.at[0])
    load_rout = pltpu.make_async_copy(router, rout, load_sem.at[1])
    load_pk = pltpu.make_async_copy(picks, pk_own, load_sem.at[3])
    load_wd = pltpu.make_async_copy(w_down.at[0], wd, load_sem.at[2])
    load_wg = [
        pltpu.make_async_copy(w_gate.at[0, span(k, LOADS)], wg.at[span(k, LOADS)], wg_sem.at[k])
        for k in range(LOADS)
    ]
    load_wu = [
        pltpu.make_async_copy(w_up.at[0, span(k, LOADS)], wu.at[span(k, LOADS)], wu_sem.at[k])
        for k in range(LOADS)
    ]

    barrier = pltpu.get_barrier_semaphore()
    peers = [n - 1 - j - (n - 1 - j <= me).astype(jnp.int32) for j in range(n - 1)]
    for peer in peers:
        pl.semaphore_signal(barrier, inc=1, device_id={"dp": peer}, device_id_type=MESH)
    load_pk.start()
    load_tok.start()
    load_rout.start()
    for k in range(LOADS):
        load_wg[k].start()
        load_wu[k].start()
    load_wd.start()

    pk_out[...] = jnp.full((2, lanes), 1 << 30, jnp.int32)
    load_pk.wait()
    pk_out[:, pl.ds(0, cap)] = jnp.broadcast_to(pk_own[...], (2, cap))
    pk_in[me] = pk_out[...]
    pl.semaphore_wait(barrier, n - 1)

    def copy_of(src, dst, send_sem, recv_sem, peer):
        return pltpu.make_async_remote_copy(
            src_ref=src, dst_ref=dst, send_sem=send_sem, recv_sem=recv_sem,
            device_id={"dp": peer}, device_id_type=MESH,
        )

    def exchange(src, dst, send_sem, recv_sem, cols):
        def copy(p, q):
            return copy_of(
                src.at[p, :, :, cols], dst.at[q, :, :, cols], send_sem.at[p], recv_sem.at[q], p
            )

        return [copy(p, me) for p in peers], [copy(p, p) for p in peers]

    pk_puts = [copy_of(pk_out, pk_in.at[me], pk_send.at[p], pk_recv.at[me], p) for p in peers]
    pk_gets = [copy_of(pk_out, pk_in.at[p], pk_send.at[p], pk_recv.at[p], p) for p in peers]
    for put in pk_puts:
        put.start()

    load_tok.wait()
    load_rout.wait()
    logits = lax.dot_general(
        rout[...], tok[...], (((1,), (1,)), ((), ())), preferred_element_type=F32
    )
    e = jnp.exp(logits - jnp.max(logits, axis=0, keepdims=True))
    gates = (experts * (e / jnp.sum(e, axis=0, keepdims=True))).astype(BF16).astype(F32)

    low = me * tok_dev

    def choose(first, last):
        pk = pk_in[first:last].reshape(2 * (last - first), lanes)
        pk = jnp.concatenate([pk] * PAIRS, axis=0)
        count = pk.shape[0]
        mine = (pk >= low) & (pk < low + tok_dev)
        start = jnp.sum(jnp.where(pk < low, 1.0, 0.0), axis=1, keepdims=True).astype(jnp.int32)
        slot = lax.broadcasted_iota(jnp.int32, (count, lanes), 1) - start
        place = (pk - low + 1).astype(F32)
        row = lax.broadcasted_iota(jnp.int32, (count, 1), 0)
        want = 2 * (row // (count // PAIRS)) + row % 2
        at = jnp.sum(jnp.where(mine & (slot == want), place, 0.0), axis=1, keepdims=True)
        token_at = lax.broadcasted_iota(jnp.int32, (count, tok_dev), 1).astype(F32) + 1.0
        return jnp.where(token_at == at, 1.0, 0.0)

    x_puts, x_gets = zip(*[
        exchange(x_out, x_in, x_send.at[k], x_recv.at[k], cut(k, X_CUTS)) for k in range(X_PARTS)
    ])
    y_puts, y_gets = zip(*[
        exchange(y_out, y_in, y_send.at[k], y_recv.at[k], cut(k, Y_CUTS)) for k in range(Y_PARTS)
    ])
    turn = half - 1
    sides = (
        (n - half, n, range(turn), me < n - half),
        (0, n - half, range(turn + 1, n - 1), me >= n - half),
    )
    for first, last, js, also in sides:
        for j in js:
            pk_gets[j].wait_recv()

        @pl.when(also)
        def _():
            pk_gets[turn].wait_recv()

        size = 2 * (last - first)
        hot = choose(first, last).astype(BF16)
        for k in range(X_PARTS):
            cols = cut(k, X_CUTS)
            block = mm(hot, tok[:, cols])
            for i in range(PAIRS):
                rows = block[i * size : (i + 1) * size].astype(BF16)
                x_out[first:last, i, :, cols] = rows.reshape(last - first, 2, rows.shape[1])
            for j in js:
                x_puts[k][j].start()

            @pl.when(also)
            def _(k=k):
                x_puts[k][turn].start()

    x_in[me] = x_out[me]
    gate_of = jnp.broadcast_to(gates[:, None, :], (n, 2, tok_dev)).reshape(2 * n, tok_dev)
    spread = (choose(0, n) * jnp.concatenate([gate_of] * PAIRS, axis=0)).T.astype(BF16)

    for copy in load_wg + load_wu:
        copy.wait()
    load_wd.wait()
    for first, last, js, also in sides[::-1]:
        size = 2 * (last - first)
        gate_act = up_act = None
        for k in range(X_PARTS):
            for j in js:
                x_gets[k][j].wait_recv()

            @pl.when(also)
            def _(k=k):
                x_gets[k][turn].wait_recv()

            cols = cut(k, X_CUTS)
            x = rows_of(x_in.at[first:last], cols)
            gate_part = mm(x, wg[cols])
            up_part = mm(x, wu[cols])
            gate_act = gate_part if k == 0 else gate_act + gate_part
            up_act = up_part if k == 0 else up_act + up_part
        hidden = (gate_act / (1.0 + jnp.exp(-gate_act)) * up_act).astype(BF16)
        for k in range(Y_PARTS):
            cols = cut(k, Y_CUTS)
            block = mm(hidden, wd[:, cols])
            for i in range(PAIRS):
                rows = block[i * size : (i + 1) * size].astype(BF16)
                y_out[first:last, i, :, cols] = rows.reshape(last - first, 2, rows.shape[1])
            for j in list(reversed(js))[:2]:
                y_puts[k][j].start()

        for k in range(Y_PARTS):
            for j in list(reversed(js))[2:]:
                y_puts[k][j].start()

            @pl.when(also)
            def _(k=k):
                y_puts[k][turn].start()

    y_in[me] = y_out[me]

    for puts in [pk_puts, *x_puts]:
        for put in puts:
            put.wait_send()
    for k in range(Y_PARTS):
        for get in y_gets[k]:
            get.wait_recv()
        cols = cut(k, Y_CUTS)
        out[:, cols] = mm(spread, rows_of(y_in, cols)).astype(BF16)
    for puts in y_puts:
        for put in puts:
            put.wait_send()


def body(tokens, router, w_gate, w_up, w_down, picks):
    n = lax.axis_size("dp")
    tok_dev, width = tokens.shape
    hidden = w_gate.shape[2]
    cap = picks.shape[1]
    lanes = -(-cap // 128) * 128
    experts = router.shape[1]
    dma = pltpu.SemaphoreType.DMA
    block = pltpu.VMEM((n, PAIRS, 2, width), BF16)
    return pl.pallas_call(
        functools.partial(kernel, n),
        out_shape=pltpu.VMEM((tok_dev, width), BF16),
        in_specs=[pl.BlockSpec(memory_space=pl.ANY)] * 6,
        out_specs=pl.BlockSpec(memory_space=pltpu.VMEM),
        scratch_shapes=[
            pltpu.VMEM((tok_dev, width), BF16),
            pltpu.VMEM((experts, width), BF16),
            pltpu.VMEM((width, hidden), BF16),
            pltpu.VMEM((width, hidden), BF16),
            pltpu.VMEM((hidden, width), BF16),
            pltpu.VMEM((1, cap), jnp.int32),
            pltpu.VMEM((2, lanes), jnp.int32),
            pltpu.VMEM((n, 2, lanes), jnp.int32),
            block, block, block, block,
            dma((4,)), dma((LOADS,)), dma((LOADS,)),
            dma((n,)), dma((n,)),
            dma((X_PARTS, n)), dma((X_PARTS, n)),
            dma((Y_PARTS, n)), dma((Y_PARTS, n)),
        ],
        compiler_params=pltpu.CompilerParams(collective_id=0, has_side_effects=True),
    )(tokens, router.T, w_gate, w_up, w_down, picks)


def solution(mesh):
    return jax.shard_map(
        body,
        mesh=mesh,
        in_specs=(
            P(("rep", "dp"), None),
            P("rep", None),
            P("dp", None, None),
            P("dp", None, None),
            P("dp", None, None),
            P(("rep", "dp"), None),
        ),
        out_specs=P(("rep", "dp"), None),
        check_vma=False,
    )
```

```python
import functools

import jax
import jax.numpy as jnp
from jax import lax
from jax.experimental import pallas as pl
from jax.experimental.pallas import tpu as pltpu
from jax.sharding import PartitionSpec as P

MESH = pl.DeviceIdType.MESH
PAIRS = 3
LOADS = 4
X_CUTS = (0, 4, 8)
Y_CUTS = (0, 4, 8)
X_PARTS = len(X_CUTS) - 1
Y_PARTS = len(Y_CUTS) - 1
F32 = jnp.float32
BF16 = jnp.bfloat16


def mm(a, b):
    return jnp.dot(a, b, preferred_element_type=F32)


def mm_t(a, b):
    return lax.dot_general(a, b, (((0,), (0,)), ((), ())), preferred_element_type=F32)


def kernel(
    n, tokens, router, w_gate, w_up, w_down, picks, out,
    tok, rout, wg, wu, wd, pk_own, pk_out, pk_in, x_out, x_in, y_out, y_in,
    load_sem, wg_sem, wu_sem,
    pk_send, pk_recv, x_send, x_recv, y_send, y_recv,
):
    me = lax.axis_index("dp")
    tok_dev, width = tok.shape
    cap = picks.shape[1]
    lanes = pk_out.shape[1]
    experts = rout.shape[0]
    half = n // 2

    def span(k, parts):
        return pl.ds(k * (width // parts), width // parts)

    def cut(k, cuts):
        unit = width // cuts[-1]
        return pl.ds(cuts[k] * unit, (cuts[k + 1] - cuts[k]) * unit)

    def rows_of(ref, cols):
        groups = [ref[:, i, :, cols].reshape(2 * ref.shape[0], cols.size) for i in range(PAIRS)]
        return jnp.concatenate(groups, axis=0)

    load_tok = pltpu.make_async_copy(tokens, tok, load_sem.at[0])
    load_rout = pltpu.make_async_copy(router, rout, load_sem.at[1])
    load_pk = pltpu.make_async_copy(picks, pk_own, load_sem.at[3])
    load_wd = pltpu.make_async_copy(w_down.at[0], wd, load_sem.at[2])
    load_wg = [
        pltpu.make_async_copy(w_gate.at[0, span(k, LOADS)], wg.at[span(k, LOADS)], wg_sem.at[k])
        for k in range(LOADS)
    ]
    load_wu = [
        pltpu.make_async_copy(w_up.at[0, span(k, LOADS)], wu.at[span(k, LOADS)], wu_sem.at[k])
        for k in range(LOADS)
    ]

    load_pk.start()
    barrier = pltpu.get_barrier_semaphore()
    peers = [n - 1 - j - (n - 1 - j <= me).astype(jnp.int32) for j in range(n - 1)]
    for peer in peers:
        pl.semaphore_signal(barrier, inc=1, device_id={"dp": peer}, device_id_type=MESH)
    load_tok.start()
    load_rout.start()
    for k in range(LOADS):
        load_wg[k].start()
        load_wu[k].start()
    load_wd.start()

    pk_out[...] = jnp.full((2, lanes), 1 << 30, jnp.int32)
    load_pk.wait()
    pk_out[:, pl.ds(0, cap)] = jnp.broadcast_to(pk_own[...], (2, cap))
    pk_in[me] = pk_out[...]
    pl.semaphore_wait(barrier, n - 1)

    def copy_of(src, dst, send_sem, recv_sem, peer):
        return pltpu.make_async_remote_copy(
            src_ref=src, dst_ref=dst, send_sem=send_sem, recv_sem=recv_sem,
            device_id={"dp": peer}, device_id_type=MESH,
        )

    def exchange(src, dst, send_sem, recv_sem, cols):
        def copy(p, q):
            return copy_of(
                src.at[p, :, :, cols], dst.at[q, :, :, cols], send_sem.at[p], recv_sem.at[q], p
            )

        return [copy(p, me) for p in peers], [copy(p, p) for p in peers]

    pk_puts = [copy_of(pk_out, pk_in.at[me], pk_send.at[p], pk_recv.at[me], p) for p in peers]
    pk_gets = [copy_of(pk_out, pk_in.at[p], pk_send.at[p], pk_recv.at[p], p) for p in peers]
    for put in pk_puts:
        put.start()

    load_tok.wait()
    load_rout.wait()
    logits = lax.dot_general(
        rout[...], tok[...], (((1,), (1,)), ((), ())), preferred_element_type=F32
    )
    e = jnp.exp(logits - jnp.max(logits, axis=0, keepdims=True))
    gates = (experts * (e / jnp.sum(e, axis=0, keepdims=True))).astype(BF16).astype(F32)

    low = me * tok_dev

    def choose(first, last):
        pk = pk_in[first:last].reshape(2 * (last - first), lanes)
        pk = jnp.concatenate([pk] * PAIRS, axis=0)
        count = pk.shape[0]
        mine = (pk >= low) & (pk < low + tok_dev)
        start = jnp.sum(jnp.where(pk < low, 1.0, 0.0), axis=1, keepdims=True).astype(jnp.int32)
        slot = lax.broadcasted_iota(jnp.int32, (count, lanes), 1) - start
        place = (pk - low + 1).astype(F32)
        row = lax.broadcasted_iota(jnp.int32, (count, 1), 0)
        want = 2 * (row // (count // PAIRS)) + row % 2
        at = jnp.sum(jnp.where(mine & (slot == want), place, 0.0), axis=1, keepdims=True)
        token_at = lax.broadcasted_iota(jnp.int32, (count, tok_dev), 1).astype(F32) + 1.0
        return jnp.where(token_at == at, 1.0, 0.0)

    x_puts, x_gets = zip(*[
        exchange(x_out, x_in, x_send.at[k], x_recv.at[k], cut(k, X_CUTS)) for k in range(X_PARTS)
    ])
    y_puts, y_gets = zip(*[
        exchange(y_out, y_in, y_send.at[k], y_recv.at[k], cut(k, Y_CUTS)) for k in range(Y_PARTS)
    ])
    turn = half - 1
    sides = (
        (n - half, n, range(turn), me < n - half),
        (0, n - half, range(turn + 1, n - 1), me >= n - half),
    )
    for first, last, js, also in sides:
        for j in js:
            pk_gets[j].wait_recv()

        @pl.when(also)
        def _():
            pk_gets[turn].wait_recv()

        size = 2 * (last - first)
        hot = choose(first, last).astype(BF16)
        for k in range(X_PARTS):
            cols = cut(k, X_CUTS)
            block = mm(hot, tok[:, cols])
            for i in range(PAIRS):
                rows = block[i * size : (i + 1) * size].astype(BF16)
                x_out[first:last, i, :, cols] = rows.reshape(last - first, 2, rows.shape[1])
            for j in js:
                x_puts[k][j].start()

            @pl.when(also)
            def _(k=k):
                x_puts[k][turn].start()

    x_in[me] = x_out[me]
    gate_of = jnp.broadcast_to(gates[:, None, :], (n, 2, tok_dev)).reshape(2 * n, tok_dev)
    spread = (choose(0, n) * jnp.concatenate([gate_of] * PAIRS, axis=0)).T.astype(BF16)

    for copy in load_wg + load_wu:
        copy.wait()
    load_wd.wait()
    for first, last, js, also in sides[::-1]:
        size = 2 * (last - first)
        gate_act = up_act = None
        for k in range(X_PARTS):
            for j in js:
                x_gets[k][j].wait_recv()

            @pl.when(also)
            def _(k=k):
                x_gets[k][turn].wait_recv()

            cols = cut(k, X_CUTS)
            x = rows_of(x_in.at[first:last], cols)
            gate_part = mm(x, wg[cols])
            up_part = mm(x, wu[cols])
            gate_act = gate_part if k == 0 else gate_act + gate_part
            up_act = up_part if k == 0 else up_act + up_part
        hidden = (gate_act / (1.0 + jnp.exp(-gate_act)) * up_act).astype(BF16)
        order = [*reversed(js)]
        order = [turn, *order] if first else [*order, turn]

        def put(k, some):
            for j in some:
                if j in js:
                    y_puts[k][j].start()
                else:
                    pl.when(also)(y_puts[k][j].start)

        for k in range(Y_PARTS):
            cols = cut(k, Y_CUTS)
            block = mm(hidden, wd[:, cols])
            for i in range(PAIRS):
                rows = block[i * size : (i + 1) * size].astype(BF16)
                y_out[first:last, i, :, cols] = rows.reshape(last - first, 2, rows.shape[1])
            put(k, order[:2])
        for k in range(Y_PARTS):
            put(k, order[2:])

    y_in[me] = y_out[me]

    for puts in [pk_puts, *x_puts]:
        for put in puts:
            put.wait_send()
    for k in range(Y_PARTS):
        for get in y_gets[k]:
            get.wait_recv()
        cols = cut(k, Y_CUTS)
        out[:, cols] = mm(spread, rows_of(y_in, cols)).astype(BF16)
    for puts in y_puts:
        for put in puts:
            put.wait_send()


def body(tokens, router, w_gate, w_up, w_down, picks):
    n = lax.axis_size("dp")
    tok_dev, width = tokens.shape
    hidden = w_gate.shape[2]
    cap = picks.shape[1]
    lanes = -(-cap // 128) * 128
    experts = router.shape[1]
    dma = pltpu.SemaphoreType.DMA
    block = pltpu.VMEM((n, PAIRS, 2, width), BF16)
    return pl.pallas_call(
        functools.partial(kernel, n),
        out_shape=pltpu.VMEM((tok_dev, width), BF16),
        in_specs=[pl.BlockSpec(memory_space=pl.ANY)] * 6,
        out_specs=pl.BlockSpec(memory_space=pltpu.VMEM),
        scratch_shapes=[
            pltpu.VMEM((tok_dev, width), BF16),
            pltpu.VMEM((experts, width), BF16),
            pltpu.VMEM((width, hidden), BF16),
            pltpu.VMEM((width, hidden), BF16),
            pltpu.VMEM((hidden, width), BF16),
            pltpu.VMEM((1, cap), jnp.int32),
            pltpu.VMEM((2, lanes), jnp.int32),
            pltpu.VMEM((n, 2, lanes), jnp.int32),
            block, block, block, block,
            dma((4,)), dma((LOADS,)), dma((LOADS,)),
            dma((n,)), dma((n,)),
            dma((X_PARTS, n)), dma((X_PARTS, n)),
            dma((Y_PARTS, n)), dma((Y_PARTS, n)),
        ],
        compiler_params=pltpu.CompilerParams(collective_id=0, has_side_effects=True),
    )(tokens, router.T, w_gate, w_up, w_down, picks)


def solution(mesh):
    return jax.shard_map(
        body,
        mesh=mesh,
        in_specs=(
            P(("rep", "dp"), None),
            P("rep", None),
            P("dp", None, None),
            P("dp", None, None),
            P("dp", None, None),
            P(("rep", "dp"), None),
        ),
        out_specs=P(("rep", "dp"), None),
        check_vma=False,
    )
```
